32 devices in a mesh: row: 8 (over z, x), col: 4 (over y, core).
Axes of the slice: x: 2, y: 2, z: 4, core: 2. Of those that a mesh axis runs over, the one named last changes fastest.
Arguments:
- basis_blocks: float32 [8, 16, 262144], P(None, None, ('col', 'row')), may hold values from -6 to 6
- tile_values: bfloat16 [4, 8, 384, 128, 128], P('col', 'row'), may hold values from -0.375 to 0.375
- tile_rows: int32 [4, 8, 384], P('col', 'row'), may hold values from 0 to 511
- tile_column: int32 [4, 8, 384], P('col', 'row'), may hold values from 0 to 255
- tile_count: int32 [4, 8], P('col', 'row'), may hold values from 1 to 384, as said below
- diagonal: float32 [262144], P(('col', 'row')), may hold values from 1 to 6
Outputs:
- new_block: float32 [16, 262144], P(None, ('col', 'row'))
- coefficients: float32 [8, 16, 16], replicated
- triangle: float32 [16, 16], replicated
The draws below stay inside these ranges and needn't reach their ends.
Inputs may be any that keep to these rules, and one draw needn't show every extreme that they name: Each operator block stores tile_count tiles in its first slots; at most 384, and some block has exactly 384 in every draw. Slots past the count hold arbitrary data and are ignored.
All inputs are finite; a program needn't handle non-finite values.
Results may differ from the reference program's by a relative error of at most 0.0031.
Values may be sent and summed in bfloat16 or wider, within the bound.
A program may use at most 128 MiB of HBM per device.

```python
import math
import jax
import jax.numpy as jnp
import numpy as np
from jax import lax

RHS = 16
BLOCKS = 8
TILE = 128
TMAX = 384
ORDER = 262144
BLOCK_ROWS = 65536
BLOCK_COLS = 32768
N_ROW = 8
N_COL = 4


def draw_basis_blocks(key, part):
    return jnp.clip(jax.random.normal(key, (BLOCKS, RHS, ORDER), jnp.float32), -6.0, 6.0)


def draw_tile_count(key, part):
    divisor = 1 + jax.random.randint(key, (N_COL, N_ROW), 0, 8)
    base_count = jnp.maximum(TMAX // divisor, 1)
    hub_index = jax.random.randint(jax.random.fold_in(key, 3), (), 0, N_COL * N_ROW)
    flat_index = jnp.arange(N_COL * N_ROW, dtype=jnp.int32).reshape(N_COL, N_ROW)
    return jnp.where(flat_index == hub_index, TMAX, base_count).astype(jnp.int32)


def draw_diagonal(key, part):
    position = jnp.arange(ORDER, dtype=jnp.float32) / ORDER
    ramp = jnp.exp(math.log(3.0) * position)
    rough = jnp.exp(jax.random.uniform(key, (ORDER,), jnp.float32, 0.0, math.log(2.0)))
    return jnp.clip(ramp * rough, 1.0, 6.0)


def touch_ends(array, rng, smallest, largest):
    shape = array.shape
    place = [jax.random.randint(jax.random.fold_in(rng, axis), (), 0, shape[axis]) for axis in range(len(shape))]
    array = array.at[tuple(place)].set(smallest)
    longest = shape.index(max(shape))
    place[longest] = (place[longest] + 1) % shape[longest]
    return array.at[tuple(place)].set(largest)


def block_levels(stream_key, extent, shards, least, largest):
    def one(dim, shards_of):
        steps = jax.random.uniform(jax.random.fold_in(jax.random.fold_in(stream_key, 6), dim), (shards_of,), jnp.float32, least / len(shards), largest / len(shards))
        return jnp.repeat(jnp.exp(steps), extent[dim] // shards_of).reshape((-1,) + (1,) * (len(extent) - dim - 1))

    gain = one(*shards[0])
    for cut in shards[1:]:
        gain = gain * one(*cut)
    return gain


def rank_bounds(count, slope):
    portions = [(1 << 20) // math.isqrt(standing ** slope) + 1 for standing in range(1, count + 1)]
    width = 1 + sum(portions) // (1 << 30)
    return np.cumsum(np.array([max(1, weight // width) for weight in portions]))


def skewed_ids(stream_key, extent, amount, skew):
    listing = rank_bounds(amount, skew)
    ticket = jax.random.randint(jax.random.fold_in(stream_key, 1), extent, 0, int(listing[amount - 1]))
    rank = jnp.searchsorted(jnp.asarray(listing, jnp.int32), ticket, side="right")
    return jax.random.permutation(jax.random.fold_in(stream_key, 2), amount)[rank].astype(jnp.int32)


def gaussian(key, dims, width, reach, pieces=(), held_as=jnp.bfloat16):
    factor_of = block_levels(key, dims, pieces, -0.22, 0.18) if pieces else 1.0
    drawn = jax.random.normal(key, dims, jnp.float32) * width * factor_of
    return jnp.minimum(jnp.maximum(drawn, -reach), reach).astype(held_as)


def setup_inputs(seed: int = 0) -> dict:
    streams_of = jax.random.split(jax.random.key(seed), 7)
    return {
        "basis_blocks": draw_basis_blocks(jax.random.fold_in(streams_of[6], 71), 0),
        "tile_values": gaussian(streams_of[1], (N_COL, N_ROW, TMAX, TILE, TILE), 0.0625, 0.375, ((0, 4), (1, 8))),
        "tile_rows": touch_ends(jax.random.randint(streams_of[2], (N_COL, N_ROW, TMAX), 0, BLOCK_ROWS // 128), jax.random.fold_in(streams_of[2], 1), 0, (BLOCK_ROWS // 128) - 1).astype(jnp.int32),
        "tile_column": touch_ends(skewed_ids(streams_of[3], (N_COL, N_ROW, TMAX), BLOCK_COLS // 128, 2), jax.random.fold_in(streams_of[3], 3), 0, (BLOCK_COLS // 128) - 1).astype(jnp.int32),
        "tile_count": draw_tile_count(jax.random.fold_in(streams_of[6], 71), 0),
        "diagonal": draw_diagonal(jax.random.fold_in(streams_of[6], 71), 0),
    }


def reference(basis_blocks, tile_values, tile_rows, tile_column, tile_count, diagonal):
    col_count, row_count, tile_slots = tile_rows.shape
    rhs_width = basis_blocks.shape[1]
    total_rows = basis_blocks.shape[2]
    seg_rows = total_rows // (col_count * row_count)
    block_tiles = row_count * seg_rows // 128
    vector = basis_blocks[-1].astype(jnp.bfloat16)
    per_set = vector.reshape(rhs_width, col_count, row_count, seg_rows).transpose(2, 0, 1, 3)
    per_set = per_set.reshape(row_count, rhs_width, col_count * seg_rows // 128, 128)

    def one_block(col_index):

        def add_part(accumulated, row_index):
            xblocks = per_set[row_index]
            gathered = jnp.take(xblocks, tile_column[col_index, row_index], axis=1)
            products = jnp.einsum('stj,tji->tsi', gathered.astype(jnp.float32), tile_values[col_index, row_index].astype(jnp.float32))
            live_tiles = (jnp.arange(tile_slots, dtype=jnp.int32) < tile_count[col_index, row_index]).astype(jnp.float32)
            products = products * live_tiles[:, None, None]
            summed = jax.ops.segment_sum(products, tile_rows[col_index, row_index], num_segments=block_tiles)
            return (accumulated + summed, None)
        initial = jnp.zeros((block_tiles, rhs_width, 128), jnp.float32)
        result, unused = lax.scan(add_part, initial, jnp.arange(row_count, dtype=jnp.int32))
        return result
    blocks_out = lax.map(one_block, jnp.arange(col_count, dtype=jnp.int32))
    image_rows = blocks_out.transpose(2, 0, 1, 3).reshape(rhs_width, total_rows)
    image_rows = image_rows + diagonal[None, :] * basis_blocks[-1]
    highest = lax.Precision.HIGHEST
    coefficients = jnp.einsum('kap,bp->kab', basis_blocks, image_rows, precision=highest) / total_rows
    projected = image_rows - jnp.einsum('kab,kap->bp', coefficients, basis_blocks, precision=highest)
    gram_matrix = jnp.dot(projected, projected.T, precision=highest) / total_rows
    lower_factor = jnp.linalg.cholesky(gram_matrix)
    new_block = lax.linalg.triangular_solve(lower_factor, projected, left_side=True, lower=True)
    return (new_block, coefficients, lower_factor.T)
```

```python
import functools

import jax
import jax.numpy as jnp
from jax import lax
from jax.experimental import pallas as pl
from jax.experimental.pallas import tpu as pltpu
from jax.sharding import PartitionSpec as P

F32 = jnp.float32
BF16 = jnp.bfloat16
TILE = 128
MESH = pl.DeviceIdType.MESH
NT = (((1,), (1,)), ((), ()))
NN = (((1,), (0,)), ((), ()))


def dot(a, b, dims):
    return lax.dot_general(a, b, dims, preferred_element_type=F32)


def split(a):
    high = a.astype(BF16)
    low = (a - high.astype(F32)).astype(BF16)
    return high, low


def dot3(a, b_high, b_low, dims):
    a_high, a_low = split(a)
    rows = a.shape[0]
    both = dot(jnp.concatenate([a_high, a_low], axis=0), b_high, dims)
    return both[:rows] + both[rows:] + dot(a_high, b_low, dims)


def gather_kernel(n_col, last_ref, out_ref, pieces, send, recv, fsend, frecv):
    tiles = last_ref.shape[1] // TILE
    me = lax.axis_index("col")
    chips = n_col // 2
    chip, core = me // 2, lax.rem(me, 2)
    partner = chip * 2 + (1 - core)
    barrier = pltpu.get_barrier_semaphore()
    for d in range(1, n_col):
        pl.semaphore_signal(barrier, 1, device_id={"col": lax.rem(me + d, n_col)}, device_id_type=MESH)
    for t in range(tiles):
        pieces[me, t] = last_ref[:, t * TILE:(t + 1) * TILE].astype(BF16)
    pl.semaphore_wait(barrier, n_col - 1)

    def move(piece, s_sem, r_sem, target):
        return pltpu.make_async_remote_copy(
            src_ref=pieces.at[piece], dst_ref=pieces.at[piece], send_sem=s_sem, recv_sem=r_sem,
            device_id={"col": target}, device_id_type=MESH)

    outgoing, incoming = [], []
    for d in range(1, chips):
        there = lax.rem(chip + d, chips) * 2 + core
        source = lax.rem(chip + chips - d, chips) * 2 + core
        op = move(me, send.at[d], recv.at[d], there)
        op.start()
        outgoing.append(op)
        incoming.append((d, source, move(source, send.at[d], recv.at[d], there)))
    op = move(me, send.at[0], recv.at[0], partner)
    op.start()
    outgoing.append(op)
    for d, source, op in incoming:
        op.wait_recv()
        op = move(source, fsend.at[d], frecv.at[d], partner)
        op.start()
        outgoing.append(op)
    move(partner, send.at[0], recv.at[0], partner).wait_recv()
    for d, source, op in incoming:
        other = lax.rem(chip + chips - d, chips) * 2 + (1 - core)
        move(other, fsend.at[d], frecv.at[d], partner).wait_recv()
    for op in outgoing:
        op.wait_send()
    out_ref[...] = pieces[...]


def gather(last, n_col):
    rhs, seg = last.shape
    shape = (n_col, seg // TILE, rhs, TILE)
    sems = pltpu.SemaphoreType.DMA((max(n_col // 2, 1),))
    return pl.pallas_call(
        functools.partial(gather_kernel, n_col),
        out_shape=jax.ShapeDtypeStruct(shape, BF16),
        in_specs=[pl.BlockSpec(memory_space=pltpu.VMEM)],
        out_specs=pl.BlockSpec(memory_space=pltpu.VMEM),
        scratch_shapes=[pltpu.VMEM(shape, BF16), sems, sems, sems, sems],
        compiler_params=pltpu.CompilerParams(collective_id=0, has_side_effects=True),
        name="gather",
    )(last)


GROUP = 16


def product_kernel(rows_ref, cols_ref, count_ref, x_ref, values_ref, out_ref, acc):
    step = pl.program_id(0)
    count = count_ref[0]

    @pl.when(step == 0)
    def _():
        acc[...] = jnp.zeros_like(acc)

    @pl.when(step * GROUP < count)
    def _():
        products = []
        for g in range(GROUP):
            products.append(dot(x_ref[cols_ref[step * GROUP + g]], values_ref[g], NN))
        spare = acc.shape[0] - 1
        for g in range(GROUP):
            slot = step * GROUP + g
            row = jnp.where(slot < count, rows_ref[slot], spare)
            acc[row] += products[g]

    @pl.when(step == pl.num_programs(0) - 1)
    def _():
        out_ref[...] = acc[:out_ref.shape[0]].astype(BF16)


def product(x, values, rows, cols, count, block_tiles):
    slots = values.shape[0]
    rhs = x.shape[1]
    last_tile = x.shape[0] - 1
    rows = jnp.clip(rows, 0, block_tiles - 1)
    cols = jnp.clip(cols, 0, last_tile)
    spec = pltpu.PrefetchScalarGridSpec(
        num_scalar_prefetch=3,
        grid=(slots // GROUP,),
        in_specs=[
            pl.BlockSpec(memory_space=pltpu.VMEM),
            pl.BlockSpec((GROUP, TILE, TILE), lambda i, r, c, n: (jnp.minimum(i, (n[0] - 1) // GROUP), 0, 0)),
        ],
        out_specs=pl.BlockSpec((block_tiles, rhs, TILE), lambda i, r, c, n: (0, 0, 0)),
        scratch_shapes=[pltpu.VMEM((block_tiles + 1, rhs, TILE), F32)],
    )
    return pl.pallas_call(
        product_kernel,
        grid_spec=spec,
        out_shape=jax.ShapeDtypeStruct((block_tiles, rhs, TILE), BF16),
        compiler_params=pltpu.CompilerParams(
            dimension_semantics=("arbitrary",), vmem_limit_bytes=40 * 2**20),
        name="product",
    )(rows, cols, count, x, values)


CHUNK = 8
FAST_FIRST = (True, False)
PANEL = 1024


def finish_kernel(slow, fast, n_col, plan, part, basis_hbm, diag, new_ref, coef_ref, tri_ref,
                  basis, high, low, image, own,
                  rf, sf, rf2, rs, ss, rs2, slots_r, slots_c, gslots_r, gslots_c,
                  basis_sem, f1s, f1r, f2s, f2r, s1s, s1r, s2s, s2r, ars, arr, acs, acr):
    n_row = slow * fast
    rhs, seg = image.shape
    total = seg * n_row * n_col
    me = lax.axis_index("row")
    mc = lax.axis_index("col")
    a, b = me // fast, lax.rem(me, fast)
    outgoing = []

    load = pltpu.make_async_copy(basis_hbm, basis, basis_sem)
    load.start()
    barrier = pltpu.get_barrier_semaphore()
    for d in range(1, n_row):
        pl.semaphore_signal(barrier, 1, device_id={"row": lax.rem(me + d, n_row)}, device_id_type=MESH)
    for d in range(1, n_col):
        pl.semaphore_signal(barrier, 1, device_id={"col": lax.rem(mc + d, n_col)}, device_id_type=MESH)
    pl.semaphore_wait(barrier, n_row - 1 + n_col - 1)

    def move(src, dst, s_sem, r_sem, axis, target):
        return pltpu.make_async_remote_copy(
            src_ref=src, dst_ref=dst, send_sem=s_sem, recv_sem=r_sem,
            device_id={axis: target}, device_id_type=MESH)

    first, second = {}, {}
    for chunk, (by_fast, i) in enumerate(plan):
        span = pl.ds(chunk * CHUNK, CHUNK)
        ops = []
        if by_fast:
            for d in range(1, fast):
                peer = lax.rem(b + d, fast)
                ops.append(move(part.at[:, peer, span], rf.at[i, d - 1], f1s.at[i, d - 1], f1r.at[i, d - 1],
                                "row", a * fast + peer))
        else:
            for d in range(1, slow):
                peer = lax.rem(a + d, slow)
                ops.append(move(part.at[peer, :, span], rs.at[i, d - 1], s1s.at[i, d - 1], s1r.at[i, d - 1],
                                "row", peer * fast + b))
        for op in ops:
            op.start()
        first[chunk] = ops
        outgoing += ops

    load.wait()
    for p in range(0, seg, PANEL):
        cut = slice(p, p + PANEL)
        high[:, cut], low[:, cut] = split(basis[:, cut])

    for chunk, (by_fast, i) in enumerate(plan):
        span = slice(chunk * CHUNK, (chunk + 1) * CHUNK)
        for op in first[chunk]:
            op.wait_recv()
        ops = []
        if by_fast:
            for d in range(slow):
                peer = lax.rem(a + d, slow)
                value = part[peer, b, span].astype(F32)
                for e in range(fast - 1):
                    value = value + rf[i, e, peer].astype(F32)
                if d == 0:
                    own[span] = value
                else:
                    sf[i, d - 1] = value.astype(BF16)
                    ops.append(move(sf.at[i, d - 1], rf2.at[i, d - 1], f2s.at[i, d - 1], f2r.at[i, d - 1],
                                    "row", peer * fast + b))
        else:
            for d in range(fast):
                peer = lax.rem(b + d, fast)
                value = part[a, peer, span].astype(F32)
                for e in range(slow - 1):
                    value = value + rs[i, e, peer].astype(F32)
                if d == 0:
                    own[span] = value
                else:
                    ss[i, d - 1] = value.astype(BF16)
                    ops.append(move(ss.at[i, d - 1], rs2.at[i, d - 1], s2s.at[i, d - 1], s2r.at[i, d - 1],
                                    "row", a * fast + peer))
        for op in ops:
            op.start()
        second[chunk] = ops
        outgoing += ops

    last = basis.shape[0] - rhs
    for chunk, (by_fast, i) in enumerate(plan):
        for op in second[chunk]:
            op.wait_recv()
        for t in range(CHUNK):
            tile = chunk * CHUNK + t
            cut = slice(tile * TILE, (tile + 1) * TILE)
            value = own[tile]
            for e in range((slow if by_fast else fast) - 1):
                value = value + (rf2[i, e, t] if by_fast else rs2[i, e, t]).astype(F32)
            image[:, cut] = value + diag[:, cut] * basis[last:, cut]

    def all_sum(value, by_row, by_col, k):
        for axis, mine, n, buf, s_sem, r_sem in (
                ("row", me, n_row, by_row, ars, arr), ("col", mc, n_col, by_col, acs, acr)):
            buf[mine] = value
            ops = []
            for d in range(1, n):
                op = move(buf.at[mine], buf.at[mine], s_sem.at[k, d], r_sem.at[k, d], axis, lax.rem(mine + d, n))
                op.start()
                ops.append(op)
            for d in range(1, n):
                source = lax.rem(mine + n - d, n)
                move(buf.at[source], buf.at[source], s_sem.at[k, d], r_sem.at[k, d], axis, source).wait_recv()
            outgoing.extend(ops)
            value = buf[0]
            for j in range(1, n):
                value = value + buf[j]
        return value

    coef = jnp.zeros((rhs, basis.shape[0]), F32)
    for p in range(0, seg, PANEL):
        cut = slice(p, p + PANEL)
        coef = coef + dot3(image[:, cut], high[:, cut], low[:, cut], NT)
    coef = all_sum(coef, slots_r, slots_c, 0) * (1.0 / total)
    coef_ref[...] = coef.T

    gram = jnp.zeros((rhs, rhs), F32)
    for p in range(0, seg, PANEL):
        cut = slice(p, p + PANEL)
        proj = image[:, cut] - dot3(coef, high[:, cut], low[:, cut], NN)
        image[:, cut] = proj
        gram = gram + dot3(proj, *split(proj), NT)
    gram = jnp.concatenate([gram, jnp.zeros((rhs, TILE - rhs), F32)], axis=1)
    gram = all_sum(gram, gslots_r, gslots_c, 1) * (1.0 / total)

    left = gram[:, :rhs]
    row_id = lax.broadcasted_iota(jnp.int32, (rhs, rhs), 0)
    right = jnp.where(row_id == lax.broadcasted_iota(jnp.int32, (rhs, rhs), 1), 1.0, 0.0).astype(F32)
    for k in range(rhs):
        scale = lax.rsqrt(left[k:k + 1, k:k + 1])
        row_l, row_r = left[k:k + 1] * scale, right[k:k + 1] * scale
        column = left[:, k:k + 1] * scale
        below = row_id > k
        here = row_id == k
        left, right = (
            jnp.where(here, row_l, jnp.where(below, left - column * row_l, left)),
            jnp.where(here, row_r, jnp.where(below, right - column * row_r, right)))
    upper = lax.broadcasted_iota(jnp.int32, (rhs, rhs), 1) >= row_id
    tri_ref[...] = jnp.where(upper, left, 0.0)
    for p in range(0, seg, PANEL):
        cut = slice(p, p + PANEL)
        new_ref[:, cut] = dot3(right, *split(image[:, cut]), NN)
    for op in outgoing:
        op.wait_send()


def finish(part, basis, diag, n_row, n_col):
    rhs, seg = diag.shape[0], basis.shape[1]
    rhs = part.shape[1]
    tiles = seg // TILE
    slow = 1 << ((n_row.bit_length()) // 2)
    fast = n_row // slow
    plan, counts = [], {True: 0, False: 0}
    for chunk in range(tiles // CHUNK):
        kind = FAST_FIRST[chunk % len(FAST_FIRST)] and fast > 1
        plan.append((kind, counts[kind]))
        counts[kind] += 1
    cf, cs = max(counts[True], 1), max(counts[False], 1)
    nf, ns = max(fast - 1, 1), max(slow - 1, 1)
    block = (CHUNK, rhs, TILE)
    width = basis.shape[0]
    dma = pltpu.SemaphoreType.DMA
    vmem = pl.BlockSpec(memory_space=pltpu.VMEM)
    return pl.pallas_call(
        functools.partial(finish_kernel, slow, fast, n_col, tuple(plan)),
        out_shape=(jax.ShapeDtypeStruct((rhs, seg), F32), jax.ShapeDtypeStruct((width, rhs), F32),
                   jax.ShapeDtypeStruct((rhs, rhs), F32)),
        in_specs=[vmem, pl.BlockSpec(memory_space=pl.ANY), vmem],
        out_specs=(vmem, vmem, vmem),
        scratch_shapes=[
            pltpu.VMEM((width, seg), F32), pltpu.VMEM((width, seg), BF16), pltpu.VMEM((width, seg), BF16),
            pltpu.VMEM((rhs, seg), F32), pltpu.VMEM((tiles, rhs, TILE), F32),
            pltpu.VMEM((cf, nf, slow) + block, BF16), pltpu.VMEM((cf, ns) + block, BF16),
            pltpu.VMEM((cf, ns) + block, BF16),
            pltpu.VMEM((cs, ns, fast) + block, BF16), pltpu.VMEM((cs, nf) + block, BF16),
            pltpu.VMEM((cs, nf) + block, BF16),
            pltpu.VMEM((n_row, rhs, width), F32), pltpu.VMEM((n_col, rhs, width), F32),
            pltpu.VMEM((n_row, rhs, TILE), F32), pltpu.VMEM((n_col, rhs, TILE), F32),
            dma(()), dma((cf, nf)), dma((cf, nf)), dma((cf, ns)), dma((cf, ns)),
            dma((cs, ns)), dma((cs, ns)), dma((cs, nf)), dma((cs, nf)),
            dma((2, n_row)), dma((2, n_row)), dma((2, n_col)), dma((2, n_col)),
        ],
        compiler_params=pltpu.CompilerParams(
            collective_id=1, has_side_effects=True, vmem_limit_bytes=48 * 2**20),
        name="finish",
    )(part.reshape(slow, fast, tiles, rhs, TILE), basis, diag)


def local(n_row, n_col, basis_blocks, tile_values, tile_rows, tile_column, tile_count, diagonal):
    blocks, rhs, seg = basis_blocks.shape
    block_tiles = n_row * seg // TILE
    x = gather(basis_blocks[-1], n_col).reshape(n_col * seg // TILE, rhs, TILE)
    part = product(x, tile_values[0, 0], tile_rows[0, 0], tile_column[0, 0], tile_count[0], block_tiles)
    new_block, coef, triangle = finish(
        part, basis_blocks.reshape(blocks * rhs, seg), diagonal[None, :], n_row, n_col)
    return new_block, coef.reshape(blocks, rhs, rhs), triangle


def solution(mesh):
    in_specs = (
        P(None, None, ("col", "row")),
        P("col", "row", None, None, None),
        P("col", "row", None),
        P("col", "row", None),
        P("col", "row"),
        P(("col", "row")),
    )
    out_specs = (P(None, ("col", "row")), P(), P())
    body = functools.partial(local, mesh.shape["row"], mesh.shape["col"])
    return jax.shard_map(body, mesh=mesh, in_specs=in_specs, out_specs=out_specs, check_vma=False)
```

```python
import functools

import jax
import jax.numpy as jnp
from jax import lax
from jax.experimental import pallas as pl
from jax.experimental.pallas import tpu as pltpu
from jax.sharding import PartitionSpec as P

F32 = jnp.float32
BF16 = jnp.bfloat16
TILE = 128
PANEL = 1024
MESH = pl.DeviceIdType.MESH
NT = (((1,), (1,)), ((), ()))
NN = (((1,), (0,)), ((), ()))


def dot(a, b, dims):
    return lax.dot_general(a, b, dims, preferred_element_type=F32)


def split(a):
    high = a.astype(BF16)
    low = (a - high.astype(F32)).astype(BF16)
    return high, low


def dot3(a, b_high, b_low, dims):
    a_high, a_low = split(a)
    rows = a.shape[0]
    both = dot(jnp.concatenate([a_high, a_low], axis=0), b_high, dims)
    return both[:rows] + both[rows:] + dot(a_high, b_low, dims)


def gather_kernel(n_col, basis_hbm, out_ref, gram_ref, basis, pieces, load_sem, all_sem, send, recv, fsend, frecv):
    width, seg = basis.shape
    rhs = pieces.shape[2]
    tiles, last = seg // TILE, width - rhs
    load = pltpu.make_async_copy(basis_hbm.at[pl.ds(last, rhs)], basis.at[pl.ds(last, rhs)], load_sem)
    load.start()
    load_all = pltpu.make_async_copy(basis_hbm.at[pl.ds(0, last)], basis.at[pl.ds(0, last)], all_sem)
    load_all.start()
    me = lax.axis_index("col")
    chips = n_col // 2
    chip, core = me // 2, lax.rem(me, 2)
    partner = chip * 2 + (1 - core)
    barrier = pltpu.get_barrier_semaphore()
    for d in range(1, n_col):
        pl.semaphore_signal(barrier, 1, device_id={"col": lax.rem(me + d, n_col)}, device_id_type=MESH)
    load.wait()
    for t in range(tiles):
        pieces[me, t] = basis[last:, t * TILE:(t + 1) * TILE].astype(BF16)
    pl.semaphore_wait(barrier, n_col - 1)

    def move(piece, s_sem, r_sem, target):
        return pltpu.make_async_remote_copy(
            src_ref=pieces.at[piece], dst_ref=pieces.at[piece], send_sem=s_sem, recv_sem=r_sem,
            device_id={"col": target}, device_id_type=MESH)

    outgoing, incoming = [], []
    for d in range(1, chips):
        there = lax.rem(chip + d, chips) * 2 + core
        source = lax.rem(chip + chips - d, chips) * 2 + core
        op = move(me, send.at[d], recv.at[d], there)
        op.start()
        outgoing.append(op)
        incoming.append((d, source, move(source, send.at[d], recv.at[d], there)))
    op = move(me, send.at[0], recv.at[0], partner)
    op.start()
    outgoing.append(op)
    load_all.wait()
    main, cross = jnp.zeros((width, width), F32), jnp.zeros((width, width), F32)
    for p in range(0, seg, PANEL):
        high, low = split(basis[:, p:p + PANEL])
        main, cross = main + dot(high, high, NT), cross + dot(low, high, NT)
    gram_ref[...] = main + cross + cross.T
    for d, source, op in incoming:
        op.wait_recv()
        op = move(source, fsend.at[d], frecv.at[d], partner)
        op.start()
        outgoing.append(op)
    move(partner, send.at[0], recv.at[0], partner).wait_recv()
    for d, source, op in incoming:
        other = lax.rem(chip + chips - d, chips) * 2 + (1 - core)
        move(other, fsend.at[d], frecv.at[d], partner).wait_recv()
    for op in outgoing:
        op.wait_send()
    out_ref[...] = pieces[...]


def gather(basis, rhs, n_col):
    width, seg = basis.shape
    shape = (n_col, seg // TILE, rhs, TILE)
    sems = pltpu.SemaphoreType.DMA((max(n_col // 2, 1),))
    return pl.pallas_call(
        functools.partial(gather_kernel, n_col),
        out_shape=(jax.ShapeDtypeStruct(shape, BF16), jax.ShapeDtypeStruct((width, width), F32)),
        in_specs=[pl.BlockSpec(memory_space=pl.ANY)],
        out_specs=(pl.BlockSpec(memory_space=pltpu.VMEM),) * 2,
        scratch_shapes=[
            pltpu.VMEM((width, seg), F32), pltpu.VMEM(shape, BF16),
            pltpu.SemaphoreType.DMA(()), pltpu.SemaphoreType.DMA(()),
            sems, sems, sems, sems],
        compiler_params=pltpu.CompilerParams(collective_id=0, has_side_effects=True),
        name="gather",
    )(basis)


GROUP = 128


def product_kernel(rows_ref, cols_ref, count_ref, x_ref, values_ref, out_ref, acc):
    step = pl.program_id(0)
    count = count_ref[0]

    @pl.when(step == 0)
    def _():
        acc[...] = jnp.zeros_like(acc)

    @pl.when(step * GROUP < count)
    def _():
        products = []
        for g in range(GROUP):
            slot = step * GROUP + g
            column = jnp.where(slot < count, cols_ref[0, slot], 0)
            products.append(dot(x_ref[column], values_ref[g], NN))
        spare = acc.shape[0] - 1
        for g in range(GROUP):
            slot = step * GROUP + g
            row = jnp.where(slot < count, rows_ref[0, slot], spare)
            acc[row] += products[g]

    @pl.when(step == pl.num_programs(0) - 1)
    def _():
        out_ref[...] = acc[:out_ref.shape[0]].astype(BF16)


def product(x, values, rows, cols, count, block_tiles):
    slots = values.shape[0]
    rhs = x.shape[1]
    spec = pltpu.PrefetchScalarGridSpec(
        num_scalar_prefetch=3,
        grid=(slots // GROUP,),
        in_specs=[
            pl.BlockSpec(memory_space=pltpu.VMEM),
            pl.BlockSpec((GROUP, TILE, TILE), lambda i, r, c, n: (jnp.minimum(i, (n[0] - 1) // GROUP), 0, 0)),
        ],
        out_specs=pl.BlockSpec((block_tiles, rhs, TILE), lambda i, r, c, n: (0, 0, 0)),
        scratch_shapes=[pltpu.VMEM((block_tiles + 1, rhs, TILE), F32)],
    )
    return pl.pallas_call(
        product_kernel,
        grid_spec=spec,
        out_shape=jax.ShapeDtypeStruct((block_tiles, rhs, TILE), BF16),
        compiler_params=pltpu.CompilerParams(
            dimension_semantics=("arbitrary",), vmem_limit_bytes=40 * 2**20),
        name="product",
    )(rows, cols, count, x, values)


CHUNK = 4
FAST_FIRST = (False,) + (True,) * 7


def finish_kernel(slow, fast, n_col, plan, part, basis_hbm, diag, local_gram, new_ref, coef_ref, tri_ref,
                  basis, high, low, image, own,
                  rf, sf, rf2, rs, ss, rs2, slots_r, slots_c, part_r, part_c, whole,
                  basis_sem, f1s, f1r, f2s, f2r, s1s, s1r, s2s, s2r, ars, arr, acs, acr, g1s, g1r, g2s, g2r, g3s, g3r):
    n_row = slow * fast
    rhs, seg = image.shape
    total = seg * n_row * n_col
    me = lax.axis_index("row")
    mc = lax.axis_index("col")
    a, b = me // fast, lax.rem(me, fast)
    outgoing = []

    load = pltpu.make_async_copy(basis_hbm, basis, basis_sem)
    load.start()
    barrier = pltpu.get_barrier_semaphore()
    for d in range(1, n_row):
        pl.semaphore_signal(barrier, 1, device_id={"row": lax.rem(me + d, n_row)}, device_id_type=MESH)
    for d in range(1, n_col):
        pl.semaphore_signal(barrier, 1, device_id={"col": lax.rem(mc + d, n_col)}, device_id_type=MESH)
    pl.semaphore_wait(barrier, n_row - 1 + n_col - 1)

    def move(src, dst, s_sem, r_sem, axis, target):
        return pltpu.make_async_remote_copy(
            src_ref=src, dst_ref=dst, send_sem=s_sem, recv_sem=r_sem,
            device_id={axis: target}, device_id_type=MESH)

    reduce_ops = []
    for d in range(1, n_row):
        peer = lax.rem(me + d, n_row)
        op = move(local_gram.at[peer], part_r.at[d - 1], g1s.at[d], g1r.at[d], "row", peer)
        op.start()
        reduce_ops.append(op)
    outgoing += reduce_ops

    first, second = {}, {}
    for chunk, (by_fast, i) in enumerate(plan):
        span = pl.ds(chunk * CHUNK, CHUNK)
        ops = []
        if by_fast:
            for d in range(1, fast):
                peer = lax.rem(b + d, fast)
                ops.append(move(part.at[:, peer, span], rf.at[i, d - 1], f1s.at[i, d - 1], f1r.at[i, d - 1],
                                "row", a * fast + peer))
        else:
            for d in range(1, slow):
                peer = lax.rem(a + d, slow)
                ops.append(move(part.at[peer, :, span], rs.at[i, d - 1], s1s.at[i, d - 1], s1r.at[i, d - 1],
                                "row", peer * fast + b))
        for op in ops:
            op.start()
        first[chunk] = ops
        outgoing += ops

    load.wait()
    for p in range(0, seg, PANEL):
        cut = slice(p, p + PANEL)
        high[:, cut], low[:, cut] = split(basis[:, cut])

    for op in reduce_ops:
        op.wait_recv()
    value = local_gram[me]
    for d in range(n_row - 1):
        value = value + part_r[d]
    part_c[mc] = value
    ops = []
    for d in range(1, n_col):
        op = move(part_c.at[mc], part_c.at[mc], g2s.at[d], g2r.at[d], "col", lax.rem(mc + d, n_col))
        op.start()
        ops.append(op)
    for d in range(1, n_col):
        source = lax.rem(mc + n_col - d, n_col)
        move(part_c.at[source], part_c.at[source], g2s.at[d], g2r.at[d], "col", source).wait_recv()
    outgoing += ops
    value = part_c[0]
    for j in range(1, n_col):
        value = value + part_c[j]
    whole[me] = value
    for d in range(1, n_row):
        op = move(whole.at[me], whole.at[me], g3s.at[d], g3r.at[d], "row", lax.rem(me + d, n_row))
        op.start()
        outgoing.append(op)

    for chunk, (by_fast, i) in enumerate(plan):
        span = slice(chunk * CHUNK, (chunk + 1) * CHUNK)
        for op in first[chunk]:
            op.wait_recv()
        ops = []
        if by_fast:
            for d in range(slow):
                peer = lax.rem(a + d, slow)
                value = part[peer, b, span].astype(F32)
                for e in range(fast - 1):
                    value = value + rf[i, e, peer].astype(F32)
                if d == 0:
                    own[span] = value
                else:
                    sf[i, d - 1] = value.astype(BF16)
                    ops.append(move(sf.at[i, d - 1], rf2.at[i, d - 1], f2s.at[i, d - 1], f2r.at[i, d - 1],
                                    "row", peer * fast + b))
        else:
            for d in range(fast):
                peer = lax.rem(b + d, fast)
                value = part[a, peer, span].astype(F32)
                for e in range(slow - 1):
                    value = value + rs[i, e, peer].astype(F32)
                if d == 0:
                    own[span] = value
                else:
                    ss[i, d - 1] = value.astype(BF16)
                    ops.append(move(ss.at[i, d - 1], rs2.at[i, d - 1], s2s.at[i, d - 1], s2r.at[i, d - 1],
                                    "row", a * fast + peer))
        for op in ops:
            op.start()
        second[chunk] = ops
        outgoing += ops

    last = basis.shape[0] - rhs
    for chunk, (by_fast, i) in enumerate(plan):
        for op in second[chunk]:
            op.wait_recv()
        for t in range(CHUNK):
            tile = chunk * CHUNK + t
            cut = slice(tile * TILE, (tile + 1) * TILE)
            value = own[tile]
            for e in range((slow if by_fast else fast) - 1):
                value = value + (rf2[i, e, t] if by_fast else rs2[i, e, t]).astype(F32)
            image[:, cut] = value + diag[:, cut] * basis[last:, cut]

    def all_sum(value, by_row, by_col):
        for axis, mine, n, buf, s_sem, r_sem in (
                ("row", me, n_row, by_row, ars, arr), ("col", mc, n_col, by_col, acs, acr)):
            buf[mine] = value
            ops = []
            for d in range(1, n):
                op = move(buf.at[mine], buf.at[mine], s_sem.at[d], r_sem.at[d], axis, lax.rem(mine + d, n))
                op.start()
                ops.append(op)
            for d in range(1, n):
                source = lax.rem(mine + n - d, n)
                move(buf.at[source], buf.at[source], s_sem.at[d], r_sem.at[d], axis, source).wait_recv()
            outgoing.extend(ops)
            value = buf[0]
            for j in range(1, n):
                value = value + buf[j]
        return value

    width = basis.shape[0]
    coef = jnp.zeros((rhs, width), F32)
    gram = jnp.zeros((rhs, rhs), F32)
    for p in range(0, seg, PANEL):
        cut = slice(p, p + PANEL)
        rows = image[:, cut]
        coef = coef + dot3(rows, high[:, cut], low[:, cut], NT)
        gram = gram + dot3(rows, *split(rows), NT)
    gram = jnp.concatenate([gram, jnp.zeros((rhs, TILE - rhs), F32)], axis=1)
    sums = all_sum(jnp.concatenate([coef, gram], axis=1), slots_r, slots_c) * (1.0 / total)
    coef = sums[:, :width]
    coef_ref[...] = coef.T
    for d in range(1, n_row):
        source = lax.rem(me + n_row - d, n_row)
        move(whole.at[source], whole.at[source], g3s.at[d], g3r.at[d], "row", source).wait_recv()
    basis_gram = whole[...].reshape(width, width) * (1.0 / total)
    exact = lax.Precision.HIGHEST
    moved = lax.dot_general(coef, basis_gram, NN, precision=exact, preferred_element_type=F32) - 2.0 * coef
    gram = sums[:, width:width + rhs] + lax.dot_general(
        moved, coef, NT, precision=exact, preferred_element_type=F32)

    left = gram
    row_id = lax.broadcasted_iota(jnp.int32, (rhs, rhs), 0)
    right = jnp.where(row_id == lax.broadcasted_iota(jnp.int32, (rhs, rhs), 1), 1.0, 0.0).astype(F32)
    for k in range(rhs):
        scale = lax.rsqrt(left[k:k + 1, k:k + 1])
        row_l, row_r = left[k:k + 1] * scale, right[k:k + 1] * scale
        column = left[:, k:k + 1] * scale
        below = row_id > k
        here = row_id == k
        left, right = (
            jnp.where(here, row_l, jnp.where(below, left - column * row_l, left)),
            jnp.where(here, row_r, jnp.where(below, right - column * row_r, right)))
    upper = lax.broadcasted_iota(jnp.int32, (rhs, rhs), 1) >= row_id
    tri_ref[...] = jnp.where(upper, left, 0.0)
    for p in range(0, seg, PANEL):
        cut = slice(p, p + PANEL)
        proj = image[:, cut] - dot3(coef, high[:, cut], low[:, cut], NN)
        new_ref[:, cut] = dot3(right, *split(proj), NN)
    for op in outgoing:
        op.wait_send()


def finish(part, basis, diag, local_gram, n_row, n_col):
    seg = basis.shape[1]
    rhs = part.shape[1]
    tiles = seg // TILE
    slow = 1 << ((n_row.bit_length()) // 2)
    fast = n_row // slow
    plan, counts = [], {True: 0, False: 0}
    for chunk in range(tiles // CHUNK):
        kind = FAST_FIRST[chunk % len(FAST_FIRST)] and fast > 1
        plan.append((kind, counts[kind]))
        counts[kind] += 1
    cf, cs = max(counts[True], 1), max(counts[False], 1)
    nf, ns = max(fast - 1, 1), max(slow - 1, 1)
    block = (CHUNK, rhs, TILE)
    width = basis.shape[0]
    dma = pltpu.SemaphoreType.DMA
    vmem = pl.BlockSpec(memory_space=pltpu.VMEM)
    return pl.pallas_call(
        functools.partial(finish_kernel, slow, fast, n_col, tuple(plan)),
        out_shape=(jax.ShapeDtypeStruct((rhs, seg), F32), jax.ShapeDtypeStruct((width, rhs), F32),
                   jax.ShapeDtypeStruct((rhs, rhs), F32)),
        in_specs=[vmem, pl.BlockSpec(memory_space=pl.ANY), vmem, vmem],
        out_specs=(vmem, vmem, vmem),
        scratch_shapes=[
            pltpu.VMEM((width, seg), F32), pltpu.VMEM((width, seg), BF16), pltpu.VMEM((width, seg), BF16),
            pltpu.VMEM((rhs, seg), F32), pltpu.VMEM((tiles, rhs, TILE), F32),
            pltpu.VMEM((cf, nf, slow) + block, BF16), pltpu.VMEM((cf, ns) + block, BF16),
            pltpu.VMEM((cf, ns) + block, BF16),
            pltpu.VMEM((cs, ns, fast) + block, BF16), pltpu.VMEM((cs, nf) + block, BF16),
            pltpu.VMEM((cs, nf) + block, BF16),
            pltpu.VMEM((n_row, rhs, width + TILE), F32), pltpu.VMEM((n_col, rhs, width + TILE), F32),
            pltpu.VMEM((n_row, width // n_row, width), F32), pltpu.VMEM((n_col, width // n_row, width), F32),
            pltpu.VMEM((n_row, width // n_row, width), F32),
            dma(()), dma((cf, nf)), dma((cf, nf)), dma((cf, ns)), dma((cf, ns)),
            dma((cs, ns)), dma((cs, ns)), dma((cs, nf)), dma((cs, nf)),
            dma((n_row,)), dma((n_row,)), dma((n_col,)), dma((n_col,)),
            dma((n_row,)), dma((n_row,)), dma((n_col,)), dma((n_col,)), dma((n_row,)), dma((n_row,)),
        ],
        compiler_params=pltpu.CompilerParams(
            collective_id=1, has_side_effects=True, vmem_limit_bytes=48 * 2**20),
        name="finish",
    )(part.reshape(slow, fast, tiles, rhs, TILE), basis, diag, local_gram.reshape(n_row, width // n_row, width))


def local(n_row, n_col, basis_blocks, tile_values, tile_rows, tile_column, tile_count, diagonal):
    blocks, rhs, seg = basis_blocks.shape
    block_tiles = n_row * seg // TILE
    basis = basis_blocks.reshape(blocks * rhs, seg)
    x, local_gram = gather(basis, rhs, n_col)
    x = x.reshape(n_col * seg // TILE, rhs, TILE)
    part = product(x, tile_values.reshape(tile_values.shape[2:]), tile_rows[0], tile_column[0], tile_count.reshape(-1), block_tiles)
    new_block, coef, triangle = finish(
        part, basis, diagonal[None, :], local_gram, n_row, n_col)
    return new_block, coef.reshape(blocks, rhs, rhs), triangle


def solution(mesh):
    in_specs = (
        P(None, None, ("col", "row")),
        P("col", "row", None, None, None),
        P("col", "row", None),
        P("col", "row", None),
        P("col", "row"),
        P(("col", "row")),
    )
    out_specs = (P(None, ("col", "row")), P(), P())
    body = functools.partial(local, mesh.shape["row"], mesh.shape["col"])
    return jax.shard_map(body, mesh=mesh, in_specs=in_specs, out_specs=out_specs, check_vma=False)
```
